32 devices in a mesh: dp: 8 (over z, x), fsdp: 4 (over y, core).
Axes of the slice: x: 2, y: 2, z: 4, core: 2. Of those that a mesh axis runs over, the one named last changes fastest.
Arguments:
- latents: bfloat16 [96, 2, 4096], P('dp'), may hold values from -6 to 6
- noise: bfloat16 [96, 2, 4096], P('dp'), may hold values from -6 to 6
- behavior_velocity: bfloat16 [96, 2, 4096], P('dp'), may hold values from -6 to 6
- timestep: int32 [96, 2], P('dp'), may hold values from 0 to 9
- reward_rank_integer: int32 [96], P('dp'), may hold values from 0 to 1023
- surviving_source_index: int32 [48], replicated, may hold values from 0 to 7, as said below
- surviving_slot_index: int32 [48], replicated, may hold values from 0 to 11, as said below
- group_kept_count: int32 [12], replicated, may hold values from 1 to 24, 48 in all
- patch_input_weight: bfloat16 [64, 1536], replicated, may hold values from -0.75 to 0.75
- modulation_lookup: float32 [10, 3, 1536], replicated, may hold values from -3 to 3
- up_projection_weight: bfloat16 [1536, 8192], P(None, 'fsdp'), may hold values from -0.15625 to 0.15625
- down_projection_weight: bfloat16 [1536, 8192], P(None, 'fsdp'), may hold values from -0.0625 to 0.0625
- velocity_head_weight: bfloat16 [1536, 64], replicated, may hold values from -0.15625 to 0.15625
Outputs:
- up_weight_gradient: float32 [1536, 8192], P('dp', 'fsdp')
- down_weight_gradient: float32 [1536, 8192], P('dp', 'fsdp')
- loss: float32 [], replicated
The draws below stay inside these ranges and needn't reach their ends.
Inputs may be any that keep to these rules, and one draw needn't show every extreme that they name: `surviving_source_index`: survivors are listed by source in ascending order; survivor j is trained on dp index j // 6, and every survivor of source d is trained on dp index d or d + 1. `surviving_slot_index`: the slots of one source's survivors are distinct.
All inputs are finite; a program needn't handle non-finite values.
Results may differ from the reference program's by a relative error of at most 0.013.
Values may be sent and summed in bfloat16 or wider, within the bound.
A program may use at most 128 MiB of HBM per device.

```python
import math
import jax
import jax.numpy as jnp
import numpy as np
from jax import lax

D = 1536
FF = 8192
PATCH = 64
SEQ = 64
TRAINED_STEPS = 2
KSTEPS = 10
GROUP = 24
TRAJ_DEV = 6
SLOT_CAPACITY = 12
SURV = 48
PROMPTS = 12
N_DP = 8


def surviving_arrangement(key):
    base_key = jax.random.fold_in(key, 7)
    drifts = jax.random.randint(jax.random.fold_in(base_key, 1), (N_DP - 1,), 0, TRAJ_DEV + 1).astype(jnp.int32)
    nothing = jnp.zeros((1,), jnp.int32)
    drifts = jnp.concatenate([nothing, drifts, nothing])
    group_starts = jnp.arange(N_DP + 1, dtype=jnp.int32) * TRAJ_DEV + drifts
    positions = jnp.arange(N_DP * TRAJ_DEV, dtype=jnp.int32)
    source = jnp.sum((group_starts[None, 1:N_DP] <= positions[:, None]).astype(jnp.int32), axis=1)
    offset = positions - jnp.take(group_starts, source)
    scores = jax.random.randint(jax.random.fold_in(base_key, 2), (N_DP, SLOT_CAPACITY), 0, 1 << 20).astype(jnp.int32) * SLOT_CAPACITY + jnp.arange(SLOT_CAPACITY, dtype=jnp.int32)[None, :]
    ordering = jnp.argsort(scores, axis=1, stable=True).astype(jnp.int32)
    slot_ids = ordering[source, offset]
    return (source.astype(jnp.int32), slot_ids.astype(jnp.int32))


def draw_surviving_source_index(key, part):
    return surviving_arrangement(key)[0]


def draw_surviving_slot_index(key, part):
    return surviving_arrangement(key)[1]


def set_ends(entries, stream_key, least, top_value):
    longest = entries.shape.index(max(entries.shape))
    spots = []
    for shift in (0, 1):
        where = [jax.random.randint(jax.random.fold_in(stream_key, axis), (), 0, length) for axis, length in enumerate(entries.shape)]
        where[longest] = (where[longest] + shift) % entries.shape[longest]
        spots.append(tuple(where))
    return entries.at[spots[0]].set(least).at[spots[1]].set(top_value)


def block_levels(key, extent, shards, smallest, largest):
    gain, own = 1.0, jax.random.fold_in(key, 6)
    for axis_at, parts in shards:
        steps = jnp.exp(jax.random.uniform(jax.random.fold_in(own, axis_at), (parts,), jnp.float32, smallest / len(shards), largest / len(shards)))
        gain = gain * jnp.repeat(steps, extent[axis_at] // parts).reshape([-1 if axis == axis_at else 1 for axis in range(len(extent))])
    return gain


def split_up(amount, total, reach, skew):
    weights = [(1 << 20) // math.isqrt(rank ** skew) + 1 for rank in range(2, amount + 1)]
    surplus, given = total - reach - (amount - 1), [1] * (amount - 1)
    while surplus > 0:
        movable = [i for i in range(amount - 1) if given[i] < reach]
        pool, remaining = sum([weights[i] for i in movable]), surplus
        for i in movable:
            extra = min(reach - given[i], max(1, remaining * weights[i] // pool), surplus)
            given[i] = given[i] + extra
            surplus = surplus - extra
    return np.array([reach] + given)


def ragged(key, number_of, total, limit, skew):
    if number_of == 2:
        one = jax.random.randint(key, (), max(1, total - limit), min(limit, total - 1) + 1)
        return jnp.stack([one, total - one])
    tallies = jnp.asarray(split_up(number_of, total, limit, skew), jnp.int32)
    couples = (number_of - 1) // 2
    donor, receiver = tallies[1:1 + 2 * couples:2], tallies[2:2 + 2 * couples:2]
    room = jnp.minimum(donor - 1, limit - receiver)
    passed = jax.random.randint(jax.random.fold_in(key, 1), (couples,), 0, 1 << 20) % (room + 1)
    tallies = tallies.at[1:1 + 2 * couples:2].set(donor - passed).at[2:2 + 2 * couples:2].set(receiver + passed)
    return tallies[jax.random.permutation(jax.random.fold_in(key, 2), number_of)]


def centred(rng, extent, scale, most, cuts=(), held_as=jnp.bfloat16):
    array = jax.random.normal(rng, extent, jnp.float32) * scale
    if len(cuts) > 0:
        array = block_levels(rng, extent, cuts, -0.22, 0.18) * array
    return jnp.clip(array, min=-most, max=most).astype(held_as)


def setup_inputs(seed: int = 0) -> dict:
    keys = jax.random.split(jax.random.key(seed), 14)
    return {
        "latents": centred(keys[0], (N_DP * SLOT_CAPACITY, TRAINED_STEPS, SEQ * PATCH), 1.0, 6.0, ((0, 8),)),
        "noise": centred(keys[1], (N_DP * SLOT_CAPACITY, TRAINED_STEPS, SEQ * PATCH), 1.0, 6.0, ((0, 8),)),
        "behavior_velocity": centred(keys[2], (N_DP * SLOT_CAPACITY, TRAINED_STEPS, SEQ * PATCH), 1.0, 6.0, ((0, 8),)),
        "timestep": set_ends(jax.random.randint(keys[3], (N_DP * SLOT_CAPACITY, TRAINED_STEPS), 0, KSTEPS), jax.random.fold_in(keys[3], 1), 0, KSTEPS - 1).astype(jnp.int32),
        "reward_rank_integer": set_ends(jax.random.randint(keys[4], (N_DP * SLOT_CAPACITY,), 0, 1024), jax.random.fold_in(keys[4], 1), 0, 1023).astype(jnp.int32),
        "surviving_source_index": draw_surviving_source_index(jax.random.fold_in(keys[13], 71), 0),
        "surviving_slot_index": draw_surviving_slot_index(jax.random.fold_in(keys[13], 71), 0),
        "group_kept_count": ragged(keys[7], PROMPTS, SURV, GROUP, 2).astype(jnp.int32),
        "patch_input_weight": centred(keys[8], (PATCH, D), PATCH ** -0.5, 0.75),
        "modulation_lookup": centred(keys[9], (KSTEPS, 3, D), 0.5, 3.0, (), jnp.float32),
        "up_projection_weight": centred(keys[10], (D, FF), D ** -0.5, 0.15625, ((1, 4),)),
        "down_projection_weight": centred(keys[11], (D, FF), FF ** -0.5, 0.0625, ((1, 4),)),
        "velocity_head_weight": centred(keys[12], (D, PATCH), D ** -0.5, 0.15625),
    }


clip_range = 0.2
noise_level = 0.7
norm_eps = 1e-06

def step_ratio(indices, count):
    spacing = 1.0 / count
    level = 1.0 - indices.astype(jnp.float32) * spacing
    return jnp.sqrt(spacing * (1.0 - level + spacing) / level) / noise_level

def layer_norm(values):
    center = values - lax.optimization_barrier(jnp.mean(values, axis=-1, keepdims=True))
    variance = lax.optimization_barrier(jnp.mean(center * center, axis=-1, keepdims=True))
    inverse = lax.rsqrt(variance + norm_eps)
    return (center * inverse, inverse)

def smooth_gate(values):
    return jax.nn.gelu(values, approximate=True)

def membership_matrix(surviving_identifiers, kept_mask):
    group_ends = jnp.cumsum(kept_mask).astype(jnp.int32)
    group_starts = group_ends - kept_mask
    inside_clip_mask = (surviving_identifiers[:, None] >= group_starts[None, :]) & (surviving_identifiers[:, None] < group_ends[None, :])
    return inside_clip_mask.astype(jnp.int32)

def advantages(ranks, member_mask, kept_mask, sums):
    count = lax.optimization_barrier(jnp.sum(member_mask * kept_mask[None, :], axis=1))
    first = lax.optimization_barrier(jnp.sum(member_mask * sums[0][None, :], axis=1))
    second = lax.optimization_barrier(jnp.sum(member_mask * sums[1][None, :], axis=1))
    spread = (count * second - first * first).astype(jnp.float32)
    counts = count.astype(jnp.float32)
    deviation = jnp.sqrt(spread) / counts
    return (ranks.astype(jnp.float32) - first.astype(jnp.float32) / counts) / jnp.maximum(deviation, 1.0)

def reference(latents, noise, behavior_velocity, timestep, reward_rank_integer, surviving_source_index, surviving_slot_index, group_kept_count, patch_input_weight, modulation_lookup, up_projection_weight, down_projection_weight, velocity_head_weight):
    surviving_count = surviving_source_index.shape[0]
    picked_indices = (surviving_source_index * SLOT_CAPACITY + surviving_slot_index).astype(jnp.int32)
    ranks = jnp.take(reward_rank_integer, picked_indices)
    member_mask = membership_matrix(jnp.arange(surviving_count, dtype=jnp.int32), group_kept_count)
    sums = jnp.stack([lax.optimization_barrier(jnp.sum(member_mask * ranks[:, None], axis=0)), lax.optimization_barrier(jnp.sum(member_mask * (ranks * ranks)[:, None], axis=0))]).astype(jnp.int32)
    advantage = advantages(ranks, member_mask, group_kept_count, sums)
    width = patch_input_weight.shape[1]
    hidden_width = up_projection_weight.shape[1]
    contract = (((0,), (0,)), ((), ()))

    def visit_group(carry, index):
        up_weight_gradient, down_weight_gradient, total_count = carry
        pick = picked_indices[index]
        sample = lax.dynamic_index_in_dim(latents, pick, 0, False)
        drawn = lax.dynamic_index_in_dim(noise, pick, 0, False).astype(jnp.float32)
        target = lax.dynamic_index_in_dim(behavior_velocity, pick, 0, False).astype(jnp.float32)
        stamps = lax.dynamic_index_in_dim(timestep, pick, 0, False)
        advantage_gain = advantage[index]
        modulation = jnp.take(modulation_lookup, stamps, axis=0)
        inputs = sample.reshape(TRAINED_STEPS * SEQ, PATCH)
        embedded = jnp.dot(inputs, patch_input_weight, preferred_element_type=jnp.float32).reshape(TRAINED_STEPS, SEQ, width)
        normed, unused_value = layer_norm(embedded)
        modulated = (normed * (1.0 + modulation[:, 1][:, None]) + modulation[:, 0][:, None]).astype(jnp.bfloat16).reshape(TRAINED_STEPS * SEQ, width)
        pre = jnp.dot(modulated, up_projection_weight, preferred_element_type=jnp.float32)
        activated = smooth_gate(pre).astype(jnp.bfloat16)
        projected = lax.dot_general(activated, down_projection_weight, (((1,), (1,)), ((), ())), preferred_element_type=jnp.float32).reshape(TRAINED_STEPS, SEQ, width)
        gates = modulation[:, 2][:, None]
        mixed = embedded + gates * projected
        final, inverse = layer_norm(mixed)
        velocity = jnp.dot(final.astype(jnp.bfloat16).reshape(TRAINED_STEPS * SEQ, width), velocity_head_weight, preferred_element_type=jnp.float32).reshape(TRAINED_STEPS, SEQ * PATCH)
        coeff = step_ratio(stamps, KSTEPS)[:, None]
        error = velocity - target
        terms = coeff * drawn * error + 0.5 * coeff * coeff * error * error
        logratio = -lax.optimization_barrier(jnp.mean(terms, axis=1))
        likelihood_ratio = jnp.exp(logratio)
        clipped = jnp.clip(likelihood_ratio, 1.0 - clip_range, 1.0 + clip_range)
        plain = likelihood_ratio * advantage_gain
        bounded = clipped * advantage_gain
        unit_loss = -jnp.minimum(plain, bounded)
        live_mask = (plain <= bounded).astype(jnp.float32)
        loss_slope = (-advantage_gain * likelihood_ratio * live_mask / (surviving_count * TRAINED_STEPS))[:, None]
        dvelocity = (loss_slope * (-(coeff * drawn + coeff * coeff * error) / (SEQ * PATCH))).astype(jnp.bfloat16).reshape(TRAINED_STEPS * SEQ, PATCH)
        dfinal = lax.dot_general(dvelocity, velocity_head_weight, (((1,), (1,)), ((), ())), preferred_element_type=jnp.float32).reshape(TRAINED_STEPS, SEQ, width)
        dmixed = inverse * (dfinal - lax.optimization_barrier(jnp.mean(dfinal, axis=-1, keepdims=True)) - final * lax.optimization_barrier(jnp.mean(dfinal * final, axis=-1, keepdims=True)))
        upstream = (gates * dmixed).astype(jnp.bfloat16).reshape(TRAINED_STEPS * SEQ, width)
        down_weight_gradient = down_weight_gradient + lax.dot_general(upstream, activated, contract, preferred_element_type=jnp.float32)
        dactivated = jnp.dot(upstream, down_projection_weight, preferred_element_type=jnp.float32)
        unused_value, pull = jax.vjp(smooth_gate, pre)
        dpre = pull(dactivated)[0].astype(jnp.bfloat16)
        up_weight_gradient = up_weight_gradient + lax.dot_general(modulated, dpre, contract, preferred_element_type=jnp.float32)
        return ((up_weight_gradient, down_weight_gradient, total_count + jnp.sum(unit_loss)), None)
    group_start = (jnp.zeros((width, hidden_width), jnp.float32), jnp.zeros((width, hidden_width), jnp.float32), jnp.zeros((), jnp.float32))
    (up_weight_gradient, down_weight_gradient, total_count), unused_value = lax.scan(visit_group, group_start, jnp.arange(surviving_count, dtype=jnp.int32))
    return (up_weight_gradient, down_weight_gradient, total_count / (surviving_count * TRAINED_STEPS))
```

```python
import functools

import jax
import jax.numpy as jnp
from jax import lax
from jax.experimental import pallas as pl
from jax.experimental.pallas import tpu as pltpu
from jax.sharding import PartitionSpec as P

KSTEPS = 10


clip_range = 0.2
noise_level = 0.7
norm_eps = 1e-06


def shortened(x):

    def short(part):
        return part.astype(jnp.bfloat16) if part.dtype == jnp.float32 else part

    return jax.tree.map(short, x)


def shifted(value, axis, steps):
    count = lax.axis_size(axis)
    initial, last = (max(0, -steps), min(count, count - steps))
    return lax.ppermute(value, axis, [(source, source + steps) for source in range(initial, last)])


def step_ratio(indices, count):
    spacing = 1.0 / count
    level = 1.0 - indices.astype(jnp.float32) * spacing
    return jnp.sqrt(spacing * (1.0 - level + spacing) / level) / noise_level


def layer_norm(values):
    center = values - jnp.mean(values, axis=-1, keepdims=True)
    variance = jnp.mean(center * center, axis=-1, keepdims=True)
    inverse = lax.rsqrt(variance + norm_eps)
    return (center * inverse, inverse)


def smooth_gate(values):
    return jax.nn.gelu(values, approximate=True)


def membership_matrix(surviving_identifiers, kept_mask):
    group_ends = jnp.cumsum(kept_mask)
    group_starts = group_ends - kept_mask
    inside_clip_mask = (surviving_identifiers[:, None] >= group_starts[None, :]) & (
        surviving_identifiers[:, None] < group_ends[None, :]
    )
    return inside_clip_mask.astype(jnp.int32)


def advantages(ranks, member_mask, kept_mask, sums):
    count = jnp.sum(member_mask * kept_mask[None, :], axis=1)
    first = jnp.sum(member_mask * sums[0][None, :], axis=1)
    second = jnp.sum(member_mask * sums[1][None, :], axis=1)
    spread = (count * second - first * first).astype(jnp.float32)
    counts = count.astype(jnp.float32)
    deviation = jnp.sqrt(spread) / counts
    return (ranks.astype(jnp.float32) - first.astype(jnp.float32) / counts) / jnp.maximum(
        deviation, 1.0
    )


def ring_place(index, count):
    odd = index % 2
    return (1 - odd) * (index // 2) + odd * (count - 1 - index // 2)


def ring_index(place, count):
    back = place // (count // 2)
    return (1 - back) * (2 * place) + back * (2 * (count - 1 - place) + 1)


def gradient_ring(
    count, pieces, modulated, dpre, upstream, activated, up_out, down_out, sent, came, send_sem, recv_sem
):
    index = lax.axis_index("dp")
    place = ring_place(index, count)
    following = ring_index((place + 1) % count, count)
    preceding = ring_index((place + count - 1) % count, count)
    barrier = pltpu.get_barrier_semaphore()
    for neighbour in (following, preceding):
        pl.semaphore_signal(
            barrier, inc=1, device_id={"dp": neighbour}, device_id_type=pl.DeviceIdType.MESH
        )
    pl.semaphore_wait(barrier, 2)
    block = modulated.shape[0] // count
    span = dpre.shape[1] // pieces
    factors = ((modulated, dpre), (upstream, activated))
    partners = (following, preceding)
    outs = (up_out, down_out)

    def target(way, step):
        turn = (place + 2 * count - 1 - step) if way == 0 else (place + 1 + step)
        return ring_index(turn % count, count)

    def own(way, step, piece):
        left, right = factors[way]
        rows = pl.ds(pl.multiple_of(target(way, step) * block, block), block)
        return jnp.dot(
            left[rows, :],
            right[:, piece * span : (piece + 1) * span],
            preferred_element_type=jnp.float32,
        )

    def copy(way, step, piece):
        return pltpu.make_async_remote_copy(
            src_ref=sent.at[way, piece, step],
            dst_ref=came.at[way, piece, step],
            send_sem=send_sem.at[way, piece, step],
            recv_sem=recv_sem.at[way, piece, step],
            device_id={"dp": partners[way]},
            device_id_type=pl.DeviceIdType.MESH,
        )

    order = [(way, piece) for piece in range(pieces) for way in range(2)]
    for way, piece in order:
        sent[way, piece, 0] = own(way, 0, piece).astype(jnp.bfloat16)
        copy(way, 0, piece).start()

    def hop(step, carry):
        for way, piece in order:
            part = own(way, step, piece)
            copy(way, step - 1, piece).wait_recv()
            sent[way, piece, step] = (
                part + came[way, piece, step - 1].astype(jnp.float32)
            ).astype(jnp.bfloat16)
            copy(way, step, piece).start()
        return carry

    lax.fori_loop(1, count - 1, hop, 0)
    for way, piece in order:
        part = own(way, count - 1, piece)
        copy(way, count - 2, piece).wait_recv()
        outs[way][:, piece * span : (piece + 1) * span] = part + came[
            way, piece, count - 2
        ].astype(jnp.float32)

    def drain(step, carry):
        for way, piece in order:
            copy(way, step, piece).wait_send()
        return carry

    lax.fori_loop(0, count - 1, drain, 0)


def reduced_gradients(modulated, dpre, upstream, activated):
    count = lax.axis_size("dp")
    pieces = max(1, 32 // count)
    block = modulated.shape[0] // count
    span = dpre.shape[1] // pieces
    shape = jax.ShapeDtypeStruct((block, dpre.shape[1]), jnp.float32)
    hops = (2, pieces, count - 1)
    return pl.pallas_call(
        functools.partial(gradient_ring, count, pieces),
        out_shape=(shape, shape),
        in_specs=[pl.BlockSpec(memory_space=pltpu.VMEM)] * 4,
        out_specs=(pl.BlockSpec(memory_space=pltpu.VMEM),) * 2,
        scratch_shapes=[
            pltpu.VMEM(hops + (block, span), jnp.bfloat16),
            pltpu.VMEM(hops + (block, span), jnp.bfloat16),
            pltpu.SemaphoreType.DMA(hops),
            pltpu.SemaphoreType.DMA(hops),
        ],
        compiler_params=pltpu.CompilerParams(
            collective_id=0, has_side_effects=True, vmem_limit_bytes=56 * 1024 * 1024
        ),
        name="gradient_ring",
    )(modulated, dpre, upstream, activated)


def shards(
    latents,
    noise,
    behavior_velocity,
    timestep,
    reward_rank_integer,
    surviving_source_index,
    surviving_slot_index,
    group_kept_count,
    patch_input_weight,
    modulation_lookup,
    up_projection_weight,
    down_projection_weight,
    velocity_head_weight,
):
    owner = lax.axis_index("dp")
    owner_ranks = lax.axis_size("dp")
    surviving_count = surviving_source_index.shape[0]
    trajectory_rows = surviving_count // owner_ranks
    leading_identifier = owner * trajectory_rows
    owned_source_index = lax.dynamic_slice_in_dim(
        surviving_source_index, leading_identifier, trajectory_rows
    )
    owned_slot_index = lax.dynamic_slice_in_dim(
        surviving_slot_index, leading_identifier, trajectory_rows
    )
    slots, step_indices, values = latents.shape
    slot_ids = jnp.arange(slots, dtype=jnp.int32)
    following_leader = jnp.minimum(owner + 1, owner_ranks - 1) * trajectory_rows
    outgoing_slot_index = lax.dynamic_slice_in_dim(
        surviving_slot_index, following_leader, trajectory_rows
    )
    picks = jnp.concatenate([owned_slot_index, outgoing_slot_index])
    chosen = picks[:, None] == slot_ids[None, :]
    whole_numbers = jnp.concatenate(
        [timestep, reward_rank_integer[:, None] // 32, reward_rank_integer[:, None] % 32], axis=1
    )
    numbers = jnp.sum(jnp.where(chosen[:, :, None], whole_numbers[None], 0), axis=1)
    select = chosen.astype(jnp.bfloat16)
    wide = step_indices * values

    def picked(array):
        return jnp.dot(
            select, array.reshape(slots, wide), preferred_element_type=jnp.float32
        ).astype(jnp.bfloat16)

    packed = jnp.concatenate(
        [
            picked(latents),
            picked(noise),
            picked(behavior_velocity),
            jnp.pad(numbers, ((0, 0), (0, 128 - numbers.shape[1]))).astype(jnp.bfloat16),
        ],
        axis=1,
    )
    arrived = shifted(packed[trajectory_rows:], "dp", 1)
    member_all = membership_matrix(jnp.arange(surviving_count, dtype=jnp.int32), group_kept_count)
    here = (surviving_source_index == owner).astype(jnp.int32)
    survivor_ranks = here * jnp.sum(
        jnp.where(
            surviving_slot_index[:, None] == slot_ids[None, :], reward_rank_integer[None, :], 0
        ),
        axis=1,
    )
    partial_value = jnp.stack(
        [
            jnp.sum(member_all * survivor_ranks[:, None], axis=0),
            jnp.sum(member_all * (survivor_ranks * survivor_ranks)[:, None], axis=0),
        ]
    ).astype(jnp.int32)
    totals = lax.psum(partial_value, "dp")
    from_left = owned_source_index != owner
    gathered = jnp.where(from_left[:, None], arrived, packed[:trajectory_rows])
    samples = gathered[:, :wide]
    noises = gathered[:, wide : 2 * wide]
    olds = gathered[:, 2 * wide : 3 * wide]
    integers = gathered[:, 3 * wide :].astype(jnp.int32)
    stamps = integers[:, :step_indices]
    ranks = integers[:, step_indices] * 32 + integers[:, step_indices + 1]
    member_mask = membership_matrix(
        leading_identifier + jnp.arange(trajectory_rows, dtype=jnp.int32), group_kept_count
    )
    advantage = advantages(ranks, member_mask, group_kept_count, totals)
    patch = patch_input_weight.shape[0]
    width = patch_input_weight.shape[1]
    units = trajectory_rows * step_indices
    seq = values // patch
    rows = units * seq
    stamp_flat = stamps.reshape(units)
    modulation = jnp.take(modulation_lookup, stamp_flat, axis=0)
    embedded = jnp.dot(
        samples.reshape(rows, patch), patch_input_weight, preferred_element_type=jnp.float32
    ).reshape(units, seq, width)
    normed, unused_value = layer_norm(embedded)
    modulated = (
        (normed * (1.0 + modulation[:, 1][:, None]) + modulation[:, 0][:, None])
        .astype(jnp.bfloat16)
        .reshape(rows, width)
    )
    pre = jnp.dot(modulated, up_projection_weight, preferred_element_type=jnp.float32)
    activated = smooth_gate(pre).astype(jnp.bfloat16)
    projected = lax.dot_general(
        activated,
        down_projection_weight,
        (((1,), (1,)), ((), ())),
        preferred_element_type=jnp.float32,
    ).astype(jnp.bfloat16)
    per_unit_gain = jnp.repeat(advantage, step_indices)
    coeff = step_ratio(stamp_flat, KSTEPS)
    gates = modulation[:, 2]
    embedded_rows = embedded.reshape(rows, width)
    old_rows = olds.reshape(rows, patch)
    noise_rows = noises.reshape(rows, patch)

    def head_terms(summed, lower, count):
        row_ids = lower + jnp.arange(count, dtype=jnp.int32)
        owner_unit = row_ids // seq
        gate_rows = jnp.take(gates, owner_unit, axis=0)
        mixed = lax.dynamic_slice_in_dim(embedded_rows, lower, count) + gate_rows * summed
        final, inverse = layer_norm(mixed)
        velocity = jnp.dot(
            final.astype(jnp.bfloat16), velocity_head_weight, preferred_element_type=jnp.float32
        )
        target = lax.dynamic_slice_in_dim(old_rows, lower, count).astype(jnp.float32)
        drawn = lax.dynamic_slice_in_dim(noise_rows, lower, count).astype(jnp.float32)
        coeff_rows = jnp.take(coeff, owner_unit)[:, None]
        error = velocity - target
        terms = coeff_rows * drawn * error + 0.5 * coeff_rows * coeff_rows * error * error
        unit_member = (owner_unit[:, None] == jnp.arange(units, dtype=jnp.int32)[None, :]).astype(
            jnp.float32
        )
        unit_sums = jnp.sum(unit_member * jnp.sum(terms, axis=1)[:, None], axis=0)

        def backward(loss_slope):
            slope_rows = jnp.take(loss_slope, owner_unit)[:, None]
            dvelocity = (
                slope_rows
                * (-(coeff_rows * drawn + coeff_rows * coeff_rows * error) / (seq * patch))
            ).astype(jnp.bfloat16)
            dfinal = lax.dot_general(
                dvelocity,
                velocity_head_weight,
                (((1,), (1,)), ((), ())),
                preferred_element_type=jnp.float32,
            )
            dmixed = inverse * (
                dfinal
                - jnp.mean(dfinal, axis=-1, keepdims=True)
                - final * jnp.mean(dfinal * final, axis=-1, keepdims=True)
            )
            return (gate_rows * dmixed).astype(jnp.bfloat16)

        return (unit_sums, backward)

    share = rows // lax.axis_size("fsdp")
    lower = lax.axis_index("fsdp") * share
    summed = lax.psum_scatter(
        projected, "fsdp", scatter_dimension=0, tiled=True
    ).astype(jnp.float32)
    part_sums, backward = head_terms(summed, lower, share)
    whole_units = share % seq == 0
    unit_sums = part_sums if whole_units else lax.psum(part_sums, "fsdp")
    logratio = -unit_sums / (seq * patch)
    likelihood_ratio = jnp.exp(logratio)
    clipped = jnp.clip(likelihood_ratio, 1.0 - clip_range, 1.0 + clip_range)
    plain = likelihood_ratio * per_unit_gain
    bounded = clipped * per_unit_gain
    unit_loss = -jnp.minimum(plain, bounded)
    live_mask = (plain <= bounded).astype(jnp.float32)
    loss_slope = -per_unit_gain * likelihood_ratio * live_mask / (surviving_count * step_indices)
    if whole_units:
        unit_ids = jnp.arange(units, dtype=jnp.int32)
        mine = (unit_ids >= lower // seq) & (unit_ids < (lower + share) // seq)
        total_count = lax.psum(jnp.sum(jnp.where(mine, unit_loss, 0.0)), ("dp", "fsdp"))
    else:
        total_count = lax.psum(jnp.sum(unit_loss), "dp")
    total_count = total_count / (surviving_count * step_indices)
    upstream = lax.all_gather(backward(loss_slope), "fsdp", axis=0, tiled=True)
    dactivated = jnp.dot(upstream, down_projection_weight, preferred_element_type=jnp.float32)
    unused_value, pull = jax.vjp(smooth_gate, pre)
    dpre = pull(dactivated)[0].astype(jnp.bfloat16)
    up_gradient, down_gradient = reduced_gradients(modulated.T, dpre, upstream.T, activated)
    return (up_gradient, down_gradient, total_count)


def solution(mesh):
    return jax.shard_map(
        shards,
        mesh=mesh,
        in_specs=(
            P("dp", None, None),
            P("dp", None, None),
            P("dp", None, None),
            P("dp", None),
            P("dp"),
            P(),
            P(),
            P(),
            P(),
            P(),
            P(None, "fsdp"),
            P(None, "fsdp"),
            P(),
        ),
        out_specs=(P("dp", "fsdp"), P("dp", "fsdp"), P()),
        check_vma=False,
    )
```

```python
import functools

import jax
import jax.numpy as jnp
from jax import lax
from jax.experimental import pallas as pl
from jax.experimental.pallas import tpu as pltpu
from jax.sharding import PartitionSpec as P

KSTEPS = 10


clip_range = 0.2
noise_level = 0.7
norm_eps = 1e-06


def shortened(x):

    def short(part):
        return part.astype(jnp.bfloat16) if part.dtype == jnp.float32 else part

    return jax.tree.map(short, x)


def shifted(value, axis, steps):
    count = lax.axis_size(axis)
    initial, last = (max(0, -steps), min(count, count - steps))
    return lax.ppermute(value, axis, [(source, source + steps) for source in range(initial, last)])


def step_ratio(indices, count):
    spacing = 1.0 / count
    level = 1.0 - indices.astype(jnp.float32) * spacing
    return jnp.sqrt(spacing * (1.0 - level + spacing) / level) / noise_level


def layer_norm(values):
    center = values - jnp.mean(values, axis=-1, keepdims=True)
    variance = jnp.mean(center * center, axis=-1, keepdims=True)
    inverse = lax.rsqrt(variance + norm_eps)
    return (center * inverse, inverse)


def smooth_gate(values):
    return jax.nn.gelu(values, approximate=True)


def membership_matrix(surviving_identifiers, kept_mask):
    group_ends = jnp.cumsum(kept_mask)
    group_starts = group_ends - kept_mask
    inside_clip_mask = (surviving_identifiers[:, None] >= group_starts[None, :]) & (
        surviving_identifiers[:, None] < group_ends[None, :]
    )
    return inside_clip_mask.astype(jnp.int32)


def advantages(ranks, member_mask, kept_mask, sums):
    count = jnp.sum(member_mask * kept_mask[None, :], axis=1)
    first = jnp.sum(member_mask * sums[0][None, :], axis=1)
    second = jnp.sum(member_mask * sums[1][None, :], axis=1)
    spread = (count * second - first * first).astype(jnp.float32)
    counts = count.astype(jnp.float32)
    deviation = jnp.sqrt(spread) / counts
    return (ranks.astype(jnp.float32) - first.astype(jnp.float32) / counts) / jnp.maximum(
        deviation, 1.0
    )


def ring_place(index, count):
    odd = index % 2
    return (1 - odd) * (index // 2) + odd * (count - 1 - index // 2)


def ring_index(place, count):
    back = place // (count // 2)
    return (1 - back) * (2 * place) + back * (2 * (count - 1 - place) + 1)


def gradient_ring(
    count,
    pieces,
    modulated_rows,
    dpre,
    upstream_rows,
    activated,
    loss,
    up_out,
    down_out,
    loss_out,
    modulated,
    upstream,
    sent,
    came,
    loss_mid,
    loss_fsdp,
    loss_dp,
    send_sem,
    recv_sem,
    fsdp_send,
    fsdp_recv,
    dp_send,
    dp_recv,
):
    index = lax.axis_index("dp")
    column = lax.axis_index("fsdp")
    columns = lax.axis_size("fsdp")
    place = ring_place(index, count)
    following = ring_index((place + 1) % count, count)
    preceding = ring_index((place + count - 1) % count, count)
    barrier = pltpu.get_barrier_semaphore()

    def greet(axis, member, size):
        def one(ahead, carry):
            pl.semaphore_signal(
                barrier,
                inc=1,
                device_id={axis: (member + ahead) % size},
                device_id_type=pl.DeviceIdType.MESH,
            )
            return carry

        lax.fori_loop(1, size, one, 0)

    greet("dp", index, count)
    greet("fsdp", column, columns)
    for rows_ref, turned in ((upstream_rows, upstream), (modulated_rows, modulated)):
        for start in range(0, turned.shape[0], 256):
            turned[start : start + 256, :] = rows_ref[:, start : start + 256].T
    pl.semaphore_wait(barrier, count - 1 + columns - 1)

    def loss_copy(axis, member, size, source, slots, send, recv, ahead):
        return pltpu.make_async_remote_copy(
            src_ref=source,
            dst_ref=slots.at[ahead - 1],
            send_sem=send.at[ahead - 1],
            recv_sem=recv.at[ahead - 1],
            device_id={axis: (member + ahead) % size},
            device_id_type=pl.DeviceIdType.MESH,
        )

    fsdp_copy = functools.partial(
        loss_copy, "fsdp", column, columns, loss, loss_fsdp, fsdp_send, fsdp_recv
    )
    dp_copy = functools.partial(loss_copy, "dp", index, count, loss_mid, loss_dp, dp_send, dp_recv)

    def start_all(make, size):
        def one(ahead, carry):
            make(ahead).start()
            return carry

        lax.fori_loop(1, size, one, 0)

    def collect(make, size, first, slots):
        def one(ahead, total):
            make(ahead).wait()
            return total + slots[ahead - 1]

        return lax.fori_loop(1, size, one, first)

    start_all(fsdp_copy, columns)
    block = modulated.shape[0] // count
    span = dpre.shape[1] // pieces
    factors = ((modulated, dpre), (upstream, activated))
    partners = (following, preceding)
    outs = (up_out, down_out)

    def target(way, step):
        turn = (place + 2 * count - 1 - step) if way == 0 else (place + 1 + step)
        return ring_index(turn % count, count)

    def own(way, step, piece):
        left, right = factors[way]
        rows = pl.ds(pl.multiple_of(target(way, step) * block, block), block)
        return jnp.dot(
            left[rows, :],
            right[:, piece * span : (piece + 1) * span],
            preferred_element_type=jnp.float32,
        )

    def copy(way, step, piece):
        return pltpu.make_async_remote_copy(
            src_ref=sent.at[way, piece, step],
            dst_ref=came.at[way, piece, step],
            send_sem=send_sem.at[way, piece, step],
            recv_sem=recv_sem.at[way, piece, step],
            device_id={"dp": partners[way]},
            device_id_type=pl.DeviceIdType.MESH,
        )

    order = [(way, piece) for piece in range(pieces) for way in range(2)]
    for way, piece in order:
        sent[way, piece, 0] = own(way, 0, piece).astype(jnp.bfloat16)
        copy(way, 0, piece).start()

    def hop(step, carry):
        for way, piece in order:
            part = own(way, step, piece)
            copy(way, step - 1, piece).wait_recv()
            sent[way, piece, step] = (
                part + came[way, piece, step - 1].astype(jnp.float32)
            ).astype(jnp.bfloat16)
            copy(way, step, piece).start()
        return carry

    loss_mid[...] = collect(fsdp_copy, columns, loss[...], loss_fsdp)
    start_all(dp_copy, count)
    lax.fori_loop(1, count - 1, hop, 0)
    for way, piece in order:
        part = own(way, count - 1, piece)
        copy(way, count - 2, piece).wait_recv()
        outs[way][:, piece * span : (piece + 1) * span] = part + came[
            way, piece, count - 2
        ].astype(jnp.float32)

    def drain(step, carry):
        for way, piece in order:
            copy(way, step, piece).wait_send()
        return carry

    lax.fori_loop(0, count - 1, drain, 0)
    loss_out[...] = collect(dp_copy, count, loss_mid[...], loss_dp)


def reduced_gradients(modulated, dpre, upstream, activated, loss):
    count = lax.axis_size("dp")
    columns = lax.axis_size("fsdp")
    pieces = max(1, 32 // count)
    rows, width = modulated.shape
    block = width // count
    tile = (8, 128)
    span = dpre.shape[1] // pieces
    shape = jax.ShapeDtypeStruct((block, dpre.shape[1]), jnp.float32)
    hops = (2, pieces, count - 1)
    return pl.pallas_call(
        functools.partial(gradient_ring, count, pieces),
        out_shape=(shape, shape, jax.ShapeDtypeStruct(tile, jnp.float32)),
        in_specs=[pl.BlockSpec(memory_space=pltpu.VMEM)] * 5,
        out_specs=(pl.BlockSpec(memory_space=pltpu.VMEM),) * 3,
        scratch_shapes=[
            pltpu.VMEM((width, rows), jnp.bfloat16),
            pltpu.VMEM((width, rows), jnp.bfloat16),
            pltpu.VMEM(hops + (block, span), jnp.bfloat16),
            pltpu.VMEM(hops + (block, span), jnp.bfloat16),
            pltpu.VMEM(tile, jnp.float32),
            pltpu.VMEM((columns - 1,) + tile, jnp.float32),
            pltpu.VMEM((count - 1,) + tile, jnp.float32),
            pltpu.SemaphoreType.DMA(hops),
            pltpu.SemaphoreType.DMA(hops),
            pltpu.SemaphoreType.DMA((columns - 1,)),
            pltpu.SemaphoreType.DMA((columns - 1,)),
            pltpu.SemaphoreType.DMA((count - 1,)),
            pltpu.SemaphoreType.DMA((count - 1,)),
        ],
        compiler_params=pltpu.CompilerParams(
            collective_id=0, has_side_effects=True, vmem_limit_bytes=56 * 1024 * 1024
        ),
        name="gradient_ring",
    )(modulated, dpre, upstream, activated, jnp.broadcast_to(loss, tile))


def pair_copy(source, target, send, recv, member):
    return pltpu.make_async_remote_copy(
        src_ref=source,
        dst_ref=target,
        send_sem=send,
        recv_sem=recv,
        device_id={"fsdp": member},
        device_id_type=pl.DeviceIdType.MESH,
    )


def pair_barrier(half, line, core):
    barrier = pltpu.get_barrier_semaphore()
    others = [2 * ((line + ahead) % half) + core for ahead in range(1, half)]
    for member in [2 * line + 1 - core] + others:
        pl.semaphore_signal(
            barrier, inc=1, device_id={"fsdp": member}, device_id_type=pl.DeviceIdType.MESH
        )
    pl.semaphore_wait(barrier, half)


def scatter_kernel(half, values, out, paired, merged, came, send_a, recv_a, send_b, recv_b):
    member = lax.axis_index("fsdp")
    line, core = member // 2, member % 2
    pair_barrier(half, line, core)

    def to_pair(ahead):
        return pair_copy(
            values.at[2 * ((line + ahead) % half) + 1 - core],
            paired.at[ahead],
            send_a.at[ahead],
            recv_a.at[ahead],
            2 * line + 1 - core,
        )

    def to_line(ahead):
        return pair_copy(
            merged.at[ahead - 1],
            came.at[ahead - 1],
            send_b.at[ahead - 1],
            recv_b.at[ahead - 1],
            2 * ((line + ahead) % half) + core,
        )

    order = list(range(1, half)) + [0]
    for ahead in order:
        to_pair(ahead).start()
    for ahead in order:
        to_pair(ahead).wait_recv()
        both = values[2 * ((line + ahead) % half) + core].astype(jnp.float32) + paired[
            ahead
        ].astype(jnp.float32)
        if ahead:
            merged[ahead - 1] = both.astype(jnp.bfloat16)
            to_line(ahead).start()
        else:
            out[...] = both
    for ahead in range(1, half):
        to_line(ahead).wait_recv()
        out[...] += came[ahead - 1].astype(jnp.float32)
    for ahead in order:
        to_pair(ahead).wait_send()
        if ahead:
            to_line(ahead).wait_send()


def scattered_sums(values):
    members = lax.axis_size("fsdp")
    half = members // 2
    share = (values.shape[0] // members, values.shape[1])
    vmem = pl.BlockSpec(memory_space=pltpu.VMEM)
    return pl.pallas_call(
        functools.partial(scatter_kernel, half),
        out_shape=jax.ShapeDtypeStruct(share, jnp.float32),
        in_specs=[vmem],
        out_specs=vmem,
        scratch_shapes=[
            pltpu.VMEM((half,) + share, jnp.bfloat16),
            pltpu.VMEM((half - 1,) + share, jnp.bfloat16),
            pltpu.VMEM((half - 1,) + share, jnp.bfloat16),
            pltpu.SemaphoreType.DMA((half,)),
            pltpu.SemaphoreType.DMA((half,)),
            pltpu.SemaphoreType.DMA((half - 1,)),
            pltpu.SemaphoreType.DMA((half - 1,)),
        ],
        compiler_params=pltpu.CompilerParams(
            collective_id=1, has_side_effects=True, vmem_limit_bytes=32 * 1024 * 1024
        ),
        name="pair_scatter",
    )(values.reshape((members,) + share))


def gather_kernel(half, value, out, send_a, recv_a, send_b, recv_b):
    member = lax.axis_index("fsdp")
    line, core = member // 2, member % 2
    pair_barrier(half, line, core)

    def to_pair(ahead):
        slot = 2 * ((line + half - ahead) % half) + core
        return pair_copy(
            out.at[slot] if ahead else value,
            out.at[slot],
            send_a.at[ahead],
            recv_a.at[ahead],
            2 * line + 1 - core,
        )

    def to_line(ahead):
        return pair_copy(
            value,
            out.at[member],
            send_b.at[ahead - 1],
            recv_b.at[ahead - 1],
            2 * ((line + ahead) % half) + core,
        )

    for ahead in range(1, half):
        to_line(ahead).start()
    to_pair(0).start()
    out[member] = value[...]
    for ahead in range(1, half):
        to_line(ahead).wait_recv()
        to_pair(ahead).start()
    for ahead in range(half):
        to_pair(ahead).wait()
        if ahead:
            to_line(ahead).wait_send()


def gathered_rows(value):
    members = lax.axis_size("fsdp")
    half = members // 2
    vmem = pl.BlockSpec(memory_space=pltpu.VMEM)
    return pl.pallas_call(
        functools.partial(gather_kernel, half),
        out_shape=jax.ShapeDtypeStruct((members,) + value.shape, value.dtype),
        in_specs=[vmem],
        out_specs=vmem,
        scratch_shapes=[
            pltpu.SemaphoreType.DMA((half,)),
            pltpu.SemaphoreType.DMA((half,)),
            pltpu.SemaphoreType.DMA((half - 1,)),
            pltpu.SemaphoreType.DMA((half - 1,)),
        ],
        compiler_params=pltpu.CompilerParams(
            collective_id=2, has_side_effects=True, vmem_limit_bytes=32 * 1024 * 1024
        ),
        name="pair_gather",
    )(value).reshape(members * value.shape[0], value.shape[1])


def shards(
    latents,
    noise,
    behavior_velocity,
    timestep,
    reward_rank_integer,
    surviving_source_index,
    surviving_slot_index,
    group_kept_count,
    patch_input_weight,
    modulation_lookup,
    up_projection_weight,
    down_projection_weight,
    velocity_head_weight,
):
    owner = lax.axis_index("dp")
    owner_ranks = lax.axis_size("dp")
    surviving_count = surviving_source_index.shape[0]
    trajectory_rows = surviving_count // owner_ranks
    leading_identifier = owner * trajectory_rows
    owned_source_index = lax.dynamic_slice_in_dim(
        surviving_source_index, leading_identifier, trajectory_rows
    )
    owned_slot_index = lax.dynamic_slice_in_dim(
        surviving_slot_index, leading_identifier, trajectory_rows
    )
    slots, step_indices, values = latents.shape
    slot_ids = jnp.arange(slots, dtype=jnp.int32)
    following_leader = jnp.minimum(owner + 1, owner_ranks - 1) * trajectory_rows
    outgoing_slot_index = lax.dynamic_slice_in_dim(
        surviving_slot_index, following_leader, trajectory_rows
    )
    picks = jnp.concatenate([owned_slot_index, outgoing_slot_index])
    chosen = picks[:, None] == slot_ids[None, :]
    whole_numbers = jnp.concatenate(
        [timestep, reward_rank_integer[:, None] // 32, reward_rank_integer[:, None] % 32], axis=1
    )
    numbers = jnp.sum(jnp.where(chosen[:, :, None], whole_numbers[None], 0), axis=1)
    select = chosen.astype(jnp.bfloat16)
    wide = step_indices * values

    def picked(array):
        return jnp.dot(
            select, array.reshape(slots, wide), preferred_element_type=jnp.float32
        ).astype(jnp.bfloat16)

    packed = jnp.concatenate(
        [
            picked(latents),
            picked(noise),
            picked(behavior_velocity),
            jnp.pad(numbers, ((0, 0), (0, 128 - numbers.shape[1]))).astype(jnp.bfloat16),
        ],
        axis=1,
    )
    arrived = shifted(packed[trajectory_rows:], "dp", 1)
    member_all = membership_matrix(jnp.arange(surviving_count, dtype=jnp.int32), group_kept_count)
    here = (surviving_source_index == owner).astype(jnp.int32)
    survivor_ranks = here * jnp.sum(
        jnp.where(
            surviving_slot_index[:, None] == slot_ids[None, :], reward_rank_integer[None, :], 0
        ),
        axis=1,
    )
    partial_value = jnp.stack(
        [
            jnp.sum(member_all * survivor_ranks[:, None], axis=0),
            jnp.sum(member_all * (survivor_ranks * survivor_ranks)[:, None], axis=0),
        ]
    ).astype(jnp.int32)
    totals = lax.psum(partial_value, "dp")
    from_left = owned_source_index != owner
    gathered = jnp.where(from_left[:, None], arrived, packed[:trajectory_rows])
    samples = gathered[:, :wide]
    noises = gathered[:, wide : 2 * wide]
    olds = gathered[:, 2 * wide : 3 * wide]
    integers = gathered[:, 3 * wide :].astype(jnp.int32)
    stamps = integers[:, :step_indices]
    ranks = integers[:, step_indices] * 32 + integers[:, step_indices + 1]
    member_mask = membership_matrix(
        leading_identifier + jnp.arange(trajectory_rows, dtype=jnp.int32), group_kept_count
    )
    advantage = advantages(ranks, member_mask, group_kept_count, totals)
    patch = patch_input_weight.shape[0]
    width = patch_input_weight.shape[1]
    units = trajectory_rows * step_indices
    seq = values // patch
    rows = units * seq
    stamp_flat = stamps.reshape(units)
    modulation = jnp.take(modulation_lookup, stamp_flat, axis=0)
    embedded = jnp.dot(
        samples.reshape(rows, patch), patch_input_weight, preferred_element_type=jnp.float32
    ).reshape(units, seq, width)
    normed, unused_value = layer_norm(embedded)
    modulated = (
        (normed * (1.0 + modulation[:, 1][:, None]) + modulation[:, 0][:, None])
        .astype(jnp.bfloat16)
        .reshape(rows, width)
    )
    pre = jnp.dot(modulated, up_projection_weight, preferred_element_type=jnp.float32)
    activated = smooth_gate(pre).astype(jnp.bfloat16)
    projected = lax.dot_general(
        activated,
        down_projection_weight,
        (((1,), (1,)), ((), ())),
        preferred_element_type=jnp.float32,
    ).astype(jnp.bfloat16)
    per_unit_gain = jnp.repeat(advantage, step_indices)
    coeff = step_ratio(stamp_flat, KSTEPS)
    gates = modulation[:, 2]
    embedded_rows = embedded.reshape(rows, width)
    old_rows = olds.reshape(rows, patch)
    noise_rows = noises.reshape(rows, patch)

    def head_terms(summed, lower, count):
        row_ids = lower + jnp.arange(count, dtype=jnp.int32)
        owner_unit = row_ids // seq
        unit_member = (owner_unit[:, None] == jnp.arange(units, dtype=jnp.int32)[None, :]).astype(
            jnp.float32
        )
        gate_rows = jnp.take(gates, owner_unit, axis=0)
        mixed = lax.dynamic_slice_in_dim(embedded_rows, lower, count) + gate_rows * summed
        final, inverse = layer_norm(mixed)
        velocity = jnp.dot(
            final.astype(jnp.bfloat16), velocity_head_weight, preferred_element_type=jnp.float32
        )
        target = lax.dynamic_slice_in_dim(old_rows, lower, count).astype(jnp.float32)
        drawn = lax.dynamic_slice_in_dim(noise_rows, lower, count).astype(jnp.float32)
        coeff_rows = jnp.sum(unit_member * coeff[None, :], axis=1, keepdims=True)
        error = velocity - target
        terms = coeff_rows * drawn * error + 0.5 * coeff_rows * coeff_rows * error * error
        unit_sums = jnp.sum(unit_member * jnp.sum(terms, axis=1)[:, None], axis=0)

        def backward(loss_slope):
            slope_rows = jnp.sum(unit_member * loss_slope[None, :], axis=1, keepdims=True)
            dvelocity = (
                slope_rows
                * (-(coeff_rows * drawn + coeff_rows * coeff_rows * error) / (seq * patch))
            ).astype(jnp.bfloat16)
            dfinal = lax.dot_general(
                dvelocity,
                velocity_head_weight,
                (((1,), (1,)), ((), ())),
                preferred_element_type=jnp.float32,
            )
            dmixed = inverse * (
                dfinal
                - jnp.mean(dfinal, axis=-1, keepdims=True)
                - final * jnp.mean(dfinal * final, axis=-1, keepdims=True)
            )
            return (gate_rows * dmixed).astype(jnp.bfloat16)

        return (unit_sums, backward)

    share = rows // lax.axis_size("fsdp")
    lower = lax.axis_index("fsdp") * share
    summed = scattered_sums(projected)
    part_sums, backward = head_terms(summed, lower, share)
    whole_units = share % seq == 0
    unit_sums = part_sums if whole_units else lax.psum(part_sums, "fsdp")
    logratio = -unit_sums / (seq * patch)
    likelihood_ratio = jnp.exp(logratio)
    clipped = jnp.clip(likelihood_ratio, 1.0 - clip_range, 1.0 + clip_range)
    plain = likelihood_ratio * per_unit_gain
    bounded = clipped * per_unit_gain
    unit_loss = -jnp.minimum(plain, bounded)
    live_mask = (plain <= bounded).astype(jnp.float32)
    loss_slope = -per_unit_gain * likelihood_ratio * live_mask / (surviving_count * step_indices)
    if whole_units:
        unit_ids = jnp.arange(units, dtype=jnp.int32)
        mine = (unit_ids >= lower // seq) & (unit_ids < (lower + share) // seq)
    else:
        mine = jnp.full((units,), lower == 0)
    loss_part = jnp.sum(jnp.where(mine, unit_loss, 0.0))
    upstream = gathered_rows(backward(loss_slope))
    dactivated = jnp.dot(upstream, down_projection_weight, preferred_element_type=jnp.float32)
    unused_value, pull = jax.vjp(smooth_gate, pre)
    dpre = pull(dactivated)[0].astype(jnp.bfloat16)
    up_gradient, down_gradient, loss_sum = reduced_gradients(
        modulated, dpre, upstream, activated, loss_part
    )
    return (up_gradient, down_gradient, loss_sum[0, 0] / (surviving_count * step_indices))


def solution(mesh):
    return jax.shard_map(
        shards,
        mesh=mesh,
        in_specs=(
            P("dp", None, None),
            P("dp", None, None),
            P("dp", None, None),
            P("dp", None),
            P("dp"),
            P(),
            P(),
            P(),
            P(),
            P(),
            P(None, "fsdp"),
            P(None, "fsdp"),
            P(),
        ),
        out_specs=(P("dp", "fsdp"), P("dp", "fsdp"), P()),
        check_vma=False,
    )
```
